32 devices in a mesh: batch: 8 (over z, y), ctx: 4 (over x, core).
Axes of the slice: x: 2, y: 2, z: 4, core: 2. Of those that a mesh axis runs over, the one named last changes fastest.
Arguments:
- asked_for: bfloat16 [16, 1024, 16, 128], P('batch', 'ctx'), may hold values from -6 to 6
- offered: bfloat16 [16, 1024, 16, 128], P('batch', 'ctx'), may hold values from -6 to 6
- contents: bfloat16 [16, 1024, 16, 128], P('batch', 'ctx'), may hold values from -6 to 6
- gate_rows: bfloat16 [16, 1024, 16, 128], P('batch', 'ctx'), may hold values from -6 to 6
- out_weight: bfloat16 [2048, 2048], P('batch'), may hold values from -0.125 to 0.125
Outputs:
- block_out: bfloat16 [16, 1024, 2048], P('batch', 'ctx')
The draws below stay inside these ranges and needn't reach their ends.
All inputs are finite; a program needn't handle non-finite values.
Results may differ from the reference program's by a relative error of at most 0.006.
Values may be sent and summed in bfloat16 or wider, within the bound.
A program may use at most 128 MiB of HBM per device.

```python
import jax
import jax.numpy as jnp
from jax import lax

HEADS = 16
HEAD_SIZE = 128
BATCH = 16
TOKENS = 1024
WIDTH = 2048


def shard_levels(key, shape, shards, low, high):
    def one(dim, parts):
        heights = jax.random.uniform(jax.random.fold_in(jax.random.fold_in(key, 6), dim), (parts,), jnp.float32, low / len(shards), high / len(shards))
        return jnp.repeat(jnp.exp(heights), shape[dim] // parts).reshape((-1,) + (1,) * (len(shape) - dim - 1))

    factor_of = one(*shards[0])
    for cut in shards[1:]:
        factor_of = factor_of * one(*cut)
    return factor_of


def normal_values(rng, extent, deviation, limit, split=(), dtype=jnp.bfloat16):
    values = deviation * jax.random.normal(rng, extent, jnp.float32)
    if split:
        values = values * shard_levels(rng, extent, split, -0.22, 0.18)
    return jnp.clip(values, -limit, limit).astype(dtype)


def setup_inputs(seed: int = 0) -> dict:
    key_of = jax.random.split(jax.random.key(seed), 6)
    asked_for = normal_values(key_of[0], (BATCH, TOKENS, HEADS, HEAD_SIZE), 1.0, 6.0, ((0, 8), (1, 4)))
    offered = normal_values(key_of[1], (BATCH, TOKENS, HEADS, HEAD_SIZE), 1.0, 6.0, ((0, 8), (1, 4)))
    contents = normal_values(key_of[2], (BATCH, TOKENS, HEADS, HEAD_SIZE), 1.0, 6.0, ((0, 8), (1, 4)))
    gate_rows = normal_values(key_of[3], (BATCH, TOKENS, HEADS, HEAD_SIZE), 1.0, 6.0, ((0, 8), (1, 4)))
    out_weight = normal_values(key_of[4], (WIDTH, WIDTH), WIDTH ** -0.5, 0.125, ((0, 8),))
    return {"asked_for": asked_for, "offered": offered, "contents": contents, "gate_rows": gate_rows, "out_weight": out_weight}


def to_features(values):
    wide = values.astype(jnp.float32)
    return (jnp.where(wide > 0.0, wide + 1.0, jnp.exp(jnp.minimum(wide, 0.0)))).astype(jnp.bfloat16)


def close_heads(read, gate_rows, count):
    result = read * count ** 0.5
    result = result * jax.nn.sigmoid(gate_rows.astype(jnp.float32))
    return result.astype(jnp.bfloat16)


def ask_state(features, state, mass):
    small = lax.optimization_barrier(state.astype(jnp.bfloat16))
    top = jnp.einsum("bthd,bhde->bthe", features.astype(jnp.float32), small.astype(jnp.float32))
    bottom = jnp.einsum("bthd,bhd->bth", features.astype(jnp.float32), mass, precision=lax.Precision.HIGHEST)
    return top / (bottom + 1e-3)[..., None]


def reference(asked_for, offered, contents, gate_rows, out_weight):
    query_feature, key_feature = lax.optimization_barrier((to_features(asked_for), to_features(offered)))
    state = jnp.einsum("bthd,bthe->bhde", key_feature.astype(jnp.float32), contents.astype(jnp.float32)) / TOKENS
    mass = jnp.sum(key_feature.astype(jnp.float32), axis=1) / TOKENS
    mixed = close_heads(ask_state(query_feature, state, mass), gate_rows, TOKENS).reshape(BATCH, TOKENS, WIDTH)
    mixed = lax.optimization_barrier(mixed)
    block_out = jnp.einsum("btw,wv->btv", mixed.astype(jnp.float32), out_weight.astype(jnp.float32)).astype(jnp.bfloat16)
    return block_out
```

```python
import functools

import jax
import jax.numpy as jnp
from jax import lax
from jax.experimental import pallas as pl
from jax.experimental.pallas import tpu as pltpu
from jax.sharding import PartitionSpec as P

MESH = pl.DeviceIdType.MESH
CORES = 2
BF16, F32 = jnp.bfloat16, jnp.float32


def ring_place(block, n):
    odd = lax.rem(block, 2)
    half = block // 2
    return (1 - odd) * half + odd * (n - 1 - half)


def ring_block(place, n):
    late = place // ((n + 1) // 2)
    return (1 - late) * (2 * place) + late * (2 * (n - 1 - place) + 1)


def features(wide):
    return jnp.where(wide > 0.0, wide + 1.0, jnp.exp(jnp.minimum(wide, 0.0))).astype(BF16).astype(F32)


def kernel(
    n, members, shared,
    q_hbm, k_hbm, v_hbm, g_hbm, w_hbm, out_hbm,
    q_in, k_in, v_in, g_in, kn, vn, qn, gn,
    part_send, part_own, part_recv, mass_send, mass_own, mass_recv,
    far_send, far_recv, mass_far_send, mass_far_recv, state, mass, state_in, mass_in,
    weight, mixed, acc, out_vm,
    in_sem, out_sem, ring_send, ring_recv, mate_send, mate_recv, far_w_send, far_w_recv,
    part_ss, part_rs, far_ss, far_rs, fin_ss, fin_rs,
):
    batch, tokens, heads, size = q_in.shape
    rows, width = weight.shape[1:]
    planes = members // CORES
    count = tokens * members
    halves = batch // CORES
    b, c = lax.axis_index("batch"), lax.axis_index("ctx")
    core, plane = lax.rem(c, CORES), c // CORES
    mate = plane * CORES + (1 - core)
    p = ring_place(b, n)
    turn = 1 - 2 * core
    nxt = ring_block(lax.rem(p + turn + n, n), n)
    prv = ring_block(lax.rem(p - turn + n, n), n)

    def far(d):
        return lax.rem(plane + d, planes) * CORES + core

    loads = [
        pltpu.make_async_copy(src, dst, in_sem.at[i])
        for i, (src, dst) in enumerate(
            [(w_hbm, weight.at[b]), (k_hbm, k_in), (v_hbm, v_in), (q_hbm, q_in), (g_hbm, g_in)]
        )
    ]
    for load in loads:
        load.start()

    barrier = pltpu.get_barrier_semaphore()
    peers = [{"batch": nxt, "ctx": c}, {"batch": prv, "ctx": c}, {"batch": b, "ctx": mate}]
    peers += [{"batch": b, "ctx": far(d)} for d in range(1, planes)]
    for peer in peers:
        pl.semaphore_signal(barrier, inc=1, device_id=peer, device_id_type=MESH)
    pl.semaphore_wait(barrier, len(peers))

    rest = (rows - planes * CORES * shared) // CORES
    base = planes * CORES * shared + core * rest
    sizes = ([shared] if shared else []) + [rest // 2, rest // 2]
    offsets = ([(plane * CORES + core) * shared] if shared else []) + [base, base + rest // 2]
    pieces = len(sizes)

    def piece(block, j):
        align = 16
        return weight.at[block, pl.ds(pl.multiple_of(offsets[j], align), sizes[j])]

    def copy(ref, send, recv, peer, dst=None):
        return pltpu.make_async_remote_copy(
            src_ref=ref, dst_ref=ref if dst is None else dst, send_sem=send, recv_sem=recv,
            device_id=peer, device_id_type=MESH,
        )

    def held(s):
        return ring_block(lax.rem(p - turn * (s + 1) + n, n), n)

    to_next, to_mate = {"batch": nxt, "ctx": c}, {"batch": b, "ctx": mate}
    sent = []

    def send(*args, **kw):
        one = copy(*args, **kw)
        one.start()
        sent.append(one)

    loads[0].wait()
    for j in range(pieces):
        send(piece(b, j), ring_send.at[0, j], ring_recv.at[0, j], to_next)

    steps = n - 1
    order = [(s, j) for s in range(steps) for j in range(pieces)]
    done = [0]
    crossed = [0]

    def ring_event(s, j):
        part = piece(held(s), j)
        copy(part, ring_send.at[s, j], ring_recv.at[s, j], to_next).wait_recv()
        if s + 1 < steps:
            send(part, ring_send.at[s + 1, j], ring_recv.at[s + 1, j], to_next)
        if shared and j == 0:
            for d in range(1, planes):
                send(part, far_w_send.at[s, d - 1], far_w_recv.at[s, d - 1], {"batch": b, "ctx": far(d)})
        send(part, mate_send.at[s, j], mate_recv.at[s, j], to_mate)

    def pump(k):
        for s, j in order[done[0] : done[0] + k]:
            ring_event(s, j)
        done[0] += k

    def pump_to(s, j):
        target = s * pieces + j + 1
        if target > done[0]:
            pump(min(target, len(order)) - done[0])

    def cross_to(s):
        while shared and crossed[0] <= min(s, steps - 1):
            s_now = crossed[0]
            for d in range(1, planes):
                other = lax.rem(plane - d + planes, planes)
                at = pl.multiple_of((other * CORES + core) * shared, 16)
                ref = weight.at[held(s_now), pl.ds(at, shared)]
                copy(ref, far_w_send.at[s_now, d - 1], far_w_recv.at[s_now, d - 1], {"batch": b, "ctx": far(d)}).wait_recv()
                slot = pieces + d - 1
                send(ref, mate_send.at[s_now, slot], mate_recv.at[s_now, slot], to_mate)
            crossed[0] += 1

    waited = [0]

    def mate_to(s):
        while waited[0] <= s:
            s_now = waited[0]
            for j in range(pieces):
                ref = weight.at[0, pl.ds(0, sizes[j])]
                copy(ref, mate_send.at[s_now, j], mate_recv.at[s_now, j], to_mate).wait_recv()
            if shared:
                for d in range(1, planes):
                    ref = weight.at[0, pl.ds(0, shared)]
                    slot = pieces + d - 1
                    copy(ref, mate_send.at[s_now, slot], mate_recv.at[s_now, slot], to_mate).wait_recv()
            waited[0] += 1

    chunk = 16

    def spread(src, seq, dst, at, fn):
        def one(i, _):
            t = pl.multiple_of(i * chunk, chunk)
            wide = fn(src[seq, pl.ds(t, chunk)].astype(F32))
            where = pl.multiple_of(at + t * heads, chunk * heads)
            dst[pl.ds(where, chunk * heads), :] = wide.reshape(chunk * heads, size)
            return 0

        lax.fori_loop(0, tokens // chunk, one, 0)

    group = 8
    per_seq = heads // group
    groups = halves * per_seq

    def one_group(part, masses, g):
        h0 = (g % per_seq) * group
        for i in range(group):
            k = kn[pl.ds(h0 + i, tokens, stride=heads), :]
            v = vn[pl.ds(h0 + i, tokens, stride=heads), :]
            part[g * group + i] = lax.dot_general(
                k.astype(BF16), v.astype(BF16), (((0,), (0,)), ((), ())), preferred_element_type=F32
            )
            masses[g, i : i + 1, :] = jnp.sum(k, axis=0, keepdims=True)

    loads[1].wait()
    loads[2].wait()
    for g in range(groups):
        if g % per_seq == 0:
            seq = (1 - core) * halves + g // per_seq
            spread(k_in, seq, kn, 0, features)
            spread(v_in, seq, vn, 0, lambda x: x)
        one_group(part_send, mass_send, g)
        span = pl.ds(g * group, group)
        send(part_send.at[span], part_ss.at[g, 0], part_rs.at[g, 0], to_mate, dst=part_recv.at[span])
        send(mass_send.at[g], part_ss.at[g, 1], part_rs.at[g, 1], to_mate, dst=mass_recv.at[g])
    for g in range(groups):
        if g % per_seq == 0:
            seq = core * halves + g // per_seq
            spread(k_in, seq, kn, 0, features)
            spread(v_in, seq, vn, 0, lambda x: x)
        one_group(part_own, mass_own, g)
        span = pl.ds(g * group, group)
        copy(part_send.at[span], part_ss.at[g, 0], part_rs.at[g, 0], to_mate, dst=part_recv.at[span]).wait_recv()
        copy(mass_send.at[g], part_ss.at[g, 1], part_rs.at[g, 1], to_mate, dst=mass_recv.at[g]).wait_recv()
        for i in range(g * group, (g + 1) * group):
            total = part_own[i] + part_recv[i]
            part_own[i] = total
            far_send[i] = total.astype(BF16)
        total = mass_own[g] + mass_recv[g]
        mass_own[g] = total
        mass_far_send[g] = total
        for d in range(1, planes):
            peer = {"batch": b, "ctx": far(d)}
            send(far_send.at[span], far_ss.at[g, d - 1, 0], far_rs.at[g, d - 1, 0], peer, dst=far_recv.at[d - 1, span])
            send(mass_far_send.at[g], far_ss.at[g, d - 1, 1], far_rs.at[g, d - 1, 1], peer, dst=mass_far_recv.at[d - 1, g])
        pump(1)

    loads[3].wait()
    for seq in range(batch):
        spread(q_in, seq, qn, seq * tokens * heads, features)
        pump(1)
    loads[4].wait()
    for seq in range(batch):
        spread(g_in, seq, gn, seq * tokens * heads, lambda x: 1.0 + jnp.exp(-x))
        pump(1)
    pump_to((n - 1) // 2, 0)

    scale = 1.0 / count
    for g in range(groups):
        span = pl.ds(g * group, group)
        for d in range(1, planes):
            peer = {"batch": b, "ctx": far(d)}
            copy(far_send.at[span], far_ss.at[g, d - 1, 0], far_rs.at[g, d - 1, 0], peer, dst=far_recv.at[d - 1, span]).wait_recv()
            copy(mass_far_send.at[g], far_ss.at[g, d - 1, 1], far_rs.at[g, d - 1, 1], peer, dst=mass_far_recv.at[d - 1, g]).wait_recv()
        for i in range(g * group, (g + 1) * group):
            total = part_own[i]
            for d in range(1, planes):
                total = total + far_recv[d - 1, i].astype(F32)
            state[i] = (total * scale).astype(BF16)
        total = mass_own[g]
        for d in range(1, planes):
            total = total + mass_far_recv[d - 1, g]
        mass[g] = total * scale
        send(state.at[span], fin_ss.at[g, 0], fin_rs.at[g, 0], to_mate, dst=state_in.at[span])
        send(mass.at[g], fin_ss.at[g, 1], fin_rs.at[g, 1], to_mate, dst=mass_in.at[g])

    per_block = rows // size

    def answer(state_ref, mass_ref, g, owner):
        seq = owner * halves + g // per_seq
        h0 = (g % per_seq) * group
        for i in range(group):
            h = h0 + i
            at = seq * (tokens * heads) + h
            ask = qn[pl.ds(at, tokens, stride=heads), :].astype(BF16)
            close = gn[pl.ds(at, tokens, stride=heads), :]
            top = jnp.dot(ask, state_ref[g * group + i], preferred_element_type=F32)
            row = mass_ref[g, i : i + 1, :]
            high = row.astype(BF16).astype(F32)
            both = jnp.concatenate([high, row - high], axis=1)
            both = jnp.broadcast_to(both, (size, 2 * size)).astype(BF16)
            bottom = lax.dot_general(
                jnp.concatenate([ask, ask], axis=1), both, (((1,), (1,)), ((), ())), preferred_element_type=F32
            )
            value = (top * count**0.5) / ((bottom + 1e-3) * close)
            lane = (h % per_block) * size
            where = pl.ds(pl.multiple_of(seq * tokens, tokens), tokens)
            mixed[h // per_block, where, lane : lane + size] = value.astype(BF16)

    for g in range(groups):
        answer(state, mass, g, core)
        pump(1)
    for g in range(groups):
        span = pl.ds(g * group, group)
        copy(state.at[span], fin_ss.at[g, 0], fin_rs.at[g, 0], to_mate, dst=state_in.at[span]).wait_recv()
        copy(mass.at[g], fin_ss.at[g, 1], fin_rs.at[g, 1], to_mate, dst=mass_in.at[g]).wait_recv()
        answer(state_in, mass_in, g, 1 - core)
        pump(1)

    if n % 2 == 0:
        sets = [(0, n // 2)] + [(n // 2 - i, n // 2 + i) for i in range(1, n // 2)]
    else:
        sets = [(0,)] + [(n // 2 + 1 - i, n // 2 + i) for i in range(1, n // 2 + 1)]
    tile = min(512, width)
    tiles = width // tile

    outs = []
    for which, offs in enumerate(sets):
        s = max(max(k, n - k) for k in offs if k) - 1 if any(offs) else -1
        pump_to(s + 1, 0)
        cross_to(s)
        pump_to(s + 1, 1)
        mate_to(s)
        blocks = [ring_block(lax.rem(p - turn * k + n, n), n) for k in offs]
        last = which == len(sets) - 1

        def column(at):
            cols = pl.ds(at, tile)
            left = jnp.concatenate([mixed[i] for i in blocks], axis=1)
            right = jnp.concatenate([weight[i, :, cols] for i in blocks], axis=0)
            made = jnp.dot(left, right, preferred_element_type=F32)
            if which:
                made = made + acc[:, cols]
            if last:
                out_vm[:, cols] = made.astype(BF16)
            else:
                acc[:, cols] = made

        if last:
            for t in range(tiles):
                column(t * tile)
                for seq in range(batch):
                    one = pltpu.make_async_copy(
                        out_vm.at[pl.ds(seq * tokens, tokens), pl.ds(t * tile, tile)],
                        out_hbm.at[seq, :, pl.ds(t * tile, tile)],
                        out_sem.at[t, seq],
                    )
                    one.start()
                    outs.append(one)
        else:
            lax.fori_loop(0, tiles, lambda t, _: (column(pl.multiple_of(t * tile, tile)), 0)[1], 0)
    for one in sent:
        one.wait_send()
    for one in outs:
        one.wait()


def solution(mesh):
    n, members = mesh.shape["batch"], mesh.shape["ctx"]
    planes = members // CORES

    def local(asked_for, offered, contents, gate_rows, out_weight):
        batch, tokens, heads, size = asked_for.shape
        rows, width = out_weight.shape
        shared = rows // 8 if planes == 2 else 0
        pieces = 3 if shared else 2
        half = batch * heads // CORES
        groups = half // 8
        slots = pieces + (planes - 1 if shared else 0)
        vm, dma = pltpu.VMEM, pltpu.SemaphoreType.DMA
        far = max(planes - 1, 1)
        whole = (batch, tokens, heads, size)
        flat = batch * tokens
        tiles = width // min(512, width)
        return pl.pallas_call(
            functools.partial(kernel, n, members, shared),
            out_shape=jax.ShapeDtypeStruct((batch, tokens, width), BF16),
            in_specs=[pl.BlockSpec(memory_space=pl.ANY)] * 5,
            out_specs=pl.BlockSpec(memory_space=pl.ANY),
            scratch_shapes=[
                vm(whole, BF16), vm(whole, BF16), vm(whole, BF16), vm(whole, BF16),
                vm((tokens * heads, size), F32), vm((tokens * heads, size), F32),
                vm((flat * heads, size), F32), vm((flat * heads, size), F32),
                vm((half, size, size), F32), vm((half, size, size), F32), vm((half, size, size), F32),
                vm((groups, 8, size), F32), vm((groups, 8, size), F32), vm((groups, 8, size), F32),
                vm((half, size, size), BF16), vm((far, half, size, size), BF16),
                vm((groups, 8, size), F32), vm((far, groups, 8, size), F32),
                vm((half, size, size), BF16), vm((groups, 8, size), F32),
                vm((half, size, size), BF16), vm((groups, 8, size), F32),
                vm((n, rows, width), BF16),
                vm((n, flat, rows), BF16),
                vm((flat, width), F32),
                vm((flat, width), BF16),
                dma((5,)), dma((tiles, batch)),
                dma((n - 1, pieces)), dma((n - 1, pieces)),
                dma((n - 1, slots)), dma((n - 1, slots)),
                dma((n - 1, far)), dma((n - 1, far)),
                dma((groups, 2)), dma((groups, 2)),
                dma((groups, far, 2)), dma((groups, far, 2)),
                dma((groups, 2)), dma((groups, 2)),
            ],
            compiler_params=pltpu.CompilerParams(
                collective_id=0, has_side_effects=True, vmem_limit_bytes=60 * 1024 * 1024
            ),
        )(asked_for, offered, contents, gate_rows, out_weight)

    return jax.shard_map(
        local,
        mesh=mesh,
        in_specs=(
            P("batch", "ctx", None, None),
            P("batch", "ctx", None, None),
            P("batch", "ctx", None, None),
            P("batch", "ctx", None, None),
            P("batch", None),
        ),
        out_specs=P("batch", "ctx", None),
        check_vma=False,
    )
```
